256 devices in a mesh: copy: 2 (over core), shard: 16 (over y, x), cols: 8 (over z).
Axes of the slice: x: 4, y: 4, z: 8, core: 2. Of those that a mesh axis runs over, the one named last changes fastest.
Arguments:
- train_gate: float32 [5120, 9728], P(('copy', 'shard'), 'cols'), parts along dimension 0, may hold values from -0.15625 to 0.15625
- drift_gate: float32 [5120, 9728], P(('copy', 'shard'), 'cols'), parts along dimension 0, may hold values from -6 to 6
- spread_gate: float32 [5120, 9728], P(('copy', 'shard'), 'cols'), parts along dimension 0, may hold values from 0.1 to 10
- train_up: float32 [5120, 9728], P(('copy', 'shard'), 'cols'), parts along dimension 0, may hold values from -0.15625 to 0.15625
- drift_up: float32 [5120, 9728], P(('copy', 'shard'), 'cols'), parts along dimension 0, may hold values from -6 to 6
- spread_up: float32 [5120, 9728], P(('copy', 'shard'), 'cols'), parts along dimension 0, may hold values from 0.1 to 10
- norm_train: float32 [5120], P(('copy', 'shard', 'cols')), parts along dimension 0, may hold values from 0.25 to 1.75
- norm_step: float32 [5120], P(('copy', 'shard', 'cols')), parts along dimension 0, may hold values from -0.3 to 0.3
Outputs:
- final_gate: bfloat16 [5120, 9728], P('copy', 'cols'), parts along dimension 0
- final_up: bfloat16 [5120, 9728], P('copy', 'cols'), parts along dimension 0
- column_gate: float32 [19456], P(('copy', 'cols')), parts along dimension 0
- column_up: float32 [19456], P(('copy', 'cols')), parts along dimension 0
- serve_norm: bfloat16 [5120], P('copy'), parts along dimension 0
- result_gate: float32 [5120, 9728], P(('copy', 'shard'), 'cols'), parts along dimension 0
- result_up: float32 [5120, 9728], P(('copy', 'shard'), 'cols'), parts along dimension 0
The draws below stay inside these ranges and needn't reach their ends.
There are 2 independent parts, one for each index of `copy`. The reference program is written for one: setup_inputs(seed, part) draws one part's arguments, and reference() takes and returns one part's arrays. A program takes and returns all parts, laid end to end along the dimension named above; each array names one. Nothing has to cross between parts.
All inputs are finite; a program needn't handle non-finite values.
Results may differ from the reference program's by a relative error of at most 0.0004.
Values may be sent and summed in bfloat16 or wider, within the bound.
A program may use at most 128 MiB of HBM per device.

```python
import math
import jax
import jax.numpy as jnp
from jax import lax

D_MODEL = 2560
D_INNER = 9728


def strengthened(array, rng, source, target, blocks, factor):
    owner, partner = [(jnp.arange(array.shape[position]) // (array.shape[position] // blocks)).reshape([-1 if axis == position else 1 for axis in range(array.ndim)]) for position in (source, target)]
    chosen = jax.random.permutation(rng, blocks)[partner]
    strong = (owner == chosen) | (owner == (partner + blocks // 2) % blocks)
    return jnp.where(strong, factor * array, array)


def block_scale(own_key, shape, shards, low, high):
    def one(dim, shards_of):
        draws = jax.random.uniform(jax.random.fold_in(jax.random.fold_in(own_key, 6), dim), (shards_of,), jnp.float32, low / len(shards), high / len(shards))
        return jnp.repeat(jnp.exp(draws), shape[dim] // shards_of).reshape((-1,) + (1,) * (len(shape) - dim - 1))

    factor_of = one(*shards[0])
    for cut in shards[1:]:
        factor_of = factor_of * one(*cut)
    return factor_of


def gaussian(stream_key, shape, scale, most, cuts=(), kind=jnp.bfloat16):
    factor_of = block_scale(stream_key, shape, cuts, -0.22, 0.18) if cuts else 1.0
    drawn = jax.random.normal(stream_key, shape, jnp.float32) * scale * factor_of
    return jnp.minimum(jnp.maximum(drawn, -most), most).astype(kind)


def gaussian_with(stream_key, extent, deviation, bound, cuts, heavy, kind=jnp.bfloat16):
    values = deviation * jax.random.normal(stream_key, extent, jnp.float32)
    if cuts:
        values = values * block_scale(stream_key, extent, cuts, -0.22, 0.18)
    return jnp.clip(strengthened(values, jax.random.fold_in(stream_key, 3), *heavy), -bound, bound).astype(kind)


def setup_inputs(seed: int = 0, part: int = 0) -> dict:
    arg_keys = jax.random.split(jax.random.key(seed), 9)
    part_keys = jax.random.split(jax.random.fold_in(arg_keys[8], part), 9)
    train_gate = gaussian_with(part_keys[0], (D_MODEL, D_INNER), D_MODEL ** -0.5, 0.15625, ((0, 16), (1, 8)), (0, 1, 16, 2.0), jnp.float32)
    drift_gate = gaussian(part_keys[1], (D_MODEL, D_INNER), 1.0, 6.0, ((0, 16), (1, 8)), jnp.float32)
    spread_gate = jnp.clip(jnp.exp(math.log(10.0) - 4.6051702 * jax.random.uniform(part_keys[2], (D_MODEL, D_INNER), jnp.float32) ** block_scale(part_keys[2], (D_MODEL, D_INNER), ((0, 16), (1, 8)), -0.2, 0.2)), 0.1, 10.0)
    train_up = gaussian_with(part_keys[3], (D_MODEL, D_INNER), D_MODEL ** -0.5, 0.15625, ((0, 16), (1, 8)), (0, 1, 16, 2.0), jnp.float32)
    drift_up = gaussian(part_keys[4], (D_MODEL, D_INNER), 1.0, 6.0, ((0, 16), (1, 8)), jnp.float32)
    spread_up = jnp.clip(jnp.exp(math.log(10.0) - 4.6051702 * jax.random.uniform(part_keys[5], (D_MODEL, D_INNER), jnp.float32) ** block_scale(part_keys[5], (D_MODEL, D_INNER), ((0, 16), (1, 8)), -0.2, 0.2)), 0.1, 10.0)
    norm_train = jnp.clip(1.0 + 0.15 * jax.random.normal(part_keys[6], (D_MODEL,), jnp.float32), 0.25, 1.75)
    norm_step = jnp.clip(jax.random.uniform(part_keys[7], (D_MODEL,), jnp.float32, -0.3, 0.3) * block_scale(part_keys[7], (D_MODEL,), ((0, 128),), -0.4, 0.0), -0.3, 0.3)
    return {"train_gate": train_gate, "drift_gate": drift_gate, "spread_gate": spread_gate, "train_up": train_up, "drift_up": drift_up, "spread_up": spread_up, "norm_train": norm_train, "norm_step": norm_step}


learn_rate = 0.015
decay_rate = 0.1
tiny_value = 1e-08

def reference(train_gate, drift_gate, spread_gate, train_up, drift_up, spread_up, norm_train, norm_step):
    result_gate = train_gate - learn_rate * (drift_gate / (jnp.sqrt(spread_gate) + tiny_value) + decay_rate * train_gate)
    result_up = train_up - learn_rate * (drift_up / (jnp.sqrt(spread_up) + tiny_value) + decay_rate * train_up)
    column_gate = jnp.sqrt(lax.optimization_barrier(jnp.sum(result_gate * result_gate, axis=0)))
    final_gate = (result_gate / column_gate).astype(jnp.bfloat16)
    column_up = jnp.sqrt(lax.optimization_barrier(jnp.sum(result_up * result_up, axis=0)))
    final_up = (result_up / column_up).astype(jnp.bfloat16)
    serve_norm = (norm_train + norm_step).astype(jnp.bfloat16)
    return (final_gate, final_up, column_gate, column_up, serve_norm, result_gate, result_up)
```

```python
import jax
import jax.numpy as jnp
from jax import lax
from jax.experimental import pallas as pl
from jax.experimental.pallas import tpu as pltpu
from jax.sharding import Mesh
from jax.sharding import PartitionSpec as P

MESH = pl.DeviceIdType.MESH
AXES = ("copy", "shard_0", "shard_1", "cols")
Y, X, Z = "shard_0", "shard_1", "cols"
N = 4

learn_rate = 0.015
decay_rate = 0.1
tiny_value = 1e-08

F32, BF16 = jnp.float32, jnp.bfloat16
ROWS, COLS, LANES = 160, 1216, 128
FULL = COLS // LANES
BLOCKS = 2 * FULL + 1
TAIL = COLS - FULL * LANES
FIRST = 8
PAIRS = FULL + 1


def updated(t, d, s):
    return t - learn_rate * (d / (jnp.sqrt(s) + tiny_value) + decay_rate * t)


def pieces(start, length):
    while length:
        here = min(length, LANES - start % LANES)
        yield start // LANES, start % LANES, here
        start, length = start + here, length - here


def unit_of(pair, along_x):
    if pair < FULL:
        return 2 * pair + (0 if along_x else 1), 0, ROWS
    return BLOCKS - 1, (0 if along_x else ROWS // 2), ROWS // 2


def gather_kernel(
    tg, dg, sg, tu, du, su, nt, ns,
    g, rg, ru, cg, cu, norm,
    tgv, dgv, sgv, tuv, duv, suv, ntv, nsv, stats, scale, n1, n2, dense,
    in_sem, stat_send, stat_recv, z_send, z_recv, n_send, n_recv, send, recv,
):
    x, y, z = lax.axis_index(X), lax.axis_index(Y), lax.axis_index(Z)
    me = y * N + x
    depth = n1.shape[0]
    right, left = lax.rem(x + 1, N), lax.rem(x + N - 1, N)
    up, down = lax.rem(y + 1, N), lax.rem(y + N - 1, N)

    loads = [
        pltpu.make_async_copy(a, b, in_sem.at[i])
        for i, (a, b) in enumerate(
            ((tg, tgv), (dg, dgv), (sg, sgv), (tu, tuv), (du, duv), (su, suv), (nt, ntv), (ns, nsv))
        )
    ]
    for load in loads:
        load.start()

    peers = [
        (k, {Y: lax.rem(y + k // N, N), X: lax.rem(x + k % N, N)}) for k in range(1, N * N)
    ]
    deep = [(k, {Z: lax.rem(z + k, depth)}) for k in range(1, depth)]
    barrier = pltpu.get_barrier_semaphore()
    for _, peer in peers + deep:
        pl.semaphore_signal(barrier, inc=1, device_id=peer, device_id_type=MESH)

    def remote(src, dst, s, r, peer):
        return pltpu.make_async_remote_copy(
            src_ref=src, dst_ref=dst, send_sem=s, recv_sem=r, device_id=peer, device_id_type=MESH
        )

    def sums_of(c, src, out):
        t, d, s = src
        lanes = pl.ds(pl.multiple_of(c * LANES, LANES), LANES)
        total = jnp.zeros((8, LANES), F32)
        for r in range(0, ROWS, 8):
            v = updated(t[pl.ds(r, 8), lanes], d[pl.ds(r, 8), lanes], s[pl.ds(r, 8), lanes])
            out[pl.ds(r, 8), lanes] = v
            total = total + v * v
        return jnp.sum(total, axis=0, keepdims=True)

    gate, upper = (tgv, dgv, sgv), (tuv, duv, suv)
    for load in loads[:3]:
        load.wait()
    for c in range(FIRST):
        stats[me, pl.ds(c, 1), :] = sums_of(c, gate, rg)

    def stat_copies(part, first, rows):
        return [
            remote(
                stats.at[me, pl.ds(first, rows)], stats.at[me, pl.ds(first, rows)],
                stat_send.at[part, k], stat_recv.at[part, k], peer,
            )
            for k, peer in peers
        ]

    pl.semaphore_wait(barrier, N * N - 1 + depth - 1)
    stats_a = stat_copies(0, 0, FIRST)
    for copy in stats_a:
        copy.start()

    for load in loads[3:]:
        load.wait()
    for c in range(FIRST, FULL):
        stats[me, pl.ds(c, 1), :] = sums_of(c, gate, rg)
    for c in range(FULL):
        stats[me, pl.ds(FULL + c, 1), :] = sums_of(c, upper, ru)
    tail = pl.ds(FULL * LANES, TAIL)
    tails = []
    for (t, d, s), out in ((gate, rg), (upper, ru)):
        v = updated(t[:, tail], d[:, tail], s[:, tail])
        out[:, tail] = v
        tails.append(v)
    mixed = jnp.concatenate(tails, axis=1)
    stats[me, pl.ds(BLOCKS - 1, 1), :] = jnp.sum(mixed * mixed, axis=0, keepdims=True)
    stats[me, pl.ds(BLOCKS, 24 - BLOCKS), :] = jnp.zeros((24 - BLOCKS, LANES), F32)
    stats_b = stat_copies(1, FIRST, 24 - FIRST)
    for copy in stats_b:
        copy.start()

    n1[z] = jnp.zeros((8, LANES), F32)
    n1[z, pl.ds(0, 1), pl.ds(0, 20)] = ntv[...] + nsv[...]
    over_z = [remote(n1.at[z], n1.at[z], z_send.at[k], z_recv.at[k], peer) for k, peer in deep]
    for copy in over_z:
        copy.start()

    def part_of(unit, first_row, rows, ys, xs):
        return g.at[unit, ys, xs, pl.ds(first_row, rows)]

    one = lambda i: pl.ds(i, 1)
    every = pl.ds(0, N)

    def hop(stage, pair, along_x, forward):
        c, r0, rows = unit_of(pair, along_x)
        on_x = along_x == (stage < 2)
        if on_x:
            peer = {X: right if forward else left}
            source = left if forward else right
        else:
            peer = {Y: up if forward else down}
            source = down if forward else up
        if stage == 0:
            ref = part_of(c, r0, rows, one(y), one(x))
        elif stage == 1:
            half = rows // 2
            r = r0 if forward else r0 + half
            ref = part_of(c, r, half, *((one(y), one(source)) if on_x else (one(source), one(x))))
        elif stage == 2:
            ref = part_of(c, r0, rows, *((every, one(x)) if on_x else (one(y), every)))
        else:
            half = pl.ds(0 if forward else N // 2, N // 2)
            ref = part_of(c, r0, rows, *((half, one(source)) if on_x else (one(source), half)))
        kind = (0 if along_x else 2) + (0 if forward else 1)
        return remote(ref, ref, send.at[stage, kind], recv.at[stage, pair, kind], peer)

    WAYS = [(a, f) for a in (True, False) for f in (True, False)]

    def start(stage, pair):
        for along_x, forward in WAYS:
            hop(stage, pair, along_x, forward).start()

    def arrived(stage, pair):
        for along_x, forward in WAYS:
            hop(stage, pair, along_x, forward).wait_recv()

    def take_scale(copies, first, rows):
        for copy in copies:
            copy.wait_recv()
        total = stats[0, pl.ds(first, rows), :]
        for p in range(1, N * N):
            total = total + stats[p, pl.ds(first, rows), :]
        scale[pl.ds(first, rows), :] = jnp.sqrt(total)

    def put(c):
        by = scale[pl.ds(c, 1), :]
        if c < BLOCKS - 1:
            src, at = (rg, c) if c < FULL else (ru, c - FULL)
            v = src[:, pl.ds(at * LANES, LANES)]
        else:
            v = jnp.concatenate([rg[:, tail], ru[:, tail]], axis=1)
        g[c, y, x] = (v / by).astype(BF16)

    take_scale(stats_a, 0, FIRST)
    for pair in range(FIRST // 2):
        put(2 * pair)
        put(2 * pair + 1)
        start(0, pair)
    take_scale(stats_b, FIRST, 24 - FIRST)
    for pair in range(FIRST // 2, PAIRS):
        put(2 * pair)
        if pair < FULL:
            put(2 * pair + 1)
        start(0, pair)

    for out, base, lane in ((cg, 0, 0), (cu, FULL, TAIL)):
        out[pl.ds(0, FULL), :] = scale[pl.ds(base, FULL), :]
        out[pl.ds(FULL, 1), pl.ds(0, TAIL)] = scale[pl.ds(BLOCKS - 1, 1), pl.ds(lane, TAIL)]

    for pair in range(PAIRS):
        arrived(0, pair)
        start(1, pair)

    for copy in over_z:
        copy.wait_recv()
    n2[me] = jnp.zeros((8, LANES), F32)
    for k in range(depth):
        done = 0
        for row, lane, length in pieces(20 * k, 20):
            n2[me, pl.ds(row, 1), pl.ds(lane, length)] = n1[k, pl.ds(0, 1), pl.ds(done, length)]
            done += length
    over_plane = [remote(n2.at[me], n2.at[me], n_send.at[k], n_recv.at[k], peer) for k, peer in peers]
    for copy in over_plane:
        copy.start()

    for pair in range(PAIRS + 1):
        if pair < PAIRS:
            arrived(1, pair)
            start(2, pair)
        if pair:
            arrived(2, pair - 1)
            start(3, pair - 1)

    for copy in over_plane:
        copy.wait_recv()
    for p in range(N * N):
        for row, lane, length in pieces(0, ROWS):
            done = 0
            for to_row, to_lane, part in pieces(ROWS * p + row * LANES, length):
                dense[pl.ds(to_row, 1), pl.ds(to_lane, part)] = n2[p, pl.ds(row, 1), pl.ds(done, part)]
                done += part
    norm[...] = dense[...].astype(BF16)

    for pair in range(PAIRS):
        arrived(3, pair)

    for copy in stats_a + stats_b + over_z + over_plane:
        copy.wait_send()
    for stage in range(4):
        half = pl.ds(0, ROWS // 2 if stage != 1 else ROWS // 4)
        xs = pl.ds(0, (1, 1, N, N // 2)[stage])
        sent = g.at[:, 0, xs, half]
        for along_x, forward in WAYS:
            kind = (0 if along_x else 2) + (0 if forward else 1)
            remote(sent, sent, send.at[stage, kind], recv.at[stage, 0, kind], {X: right}).wait_send()


def write_kernel(
    g, rg, ru, cg_in, cu_in, norm_in, fg, fu, og, ou, cg, cu, norm, tiles, out_sem, tile_sem
):
    others = [
        pltpu.make_async_copy(a, b, out_sem.at[i])
        for i, (a, b) in enumerate(
            ((rg, og), (ru, ou), (cg_in, cg), (cu_in, cu), (norm_in, norm))
        )
    ]
    for copy in others:
        copy.start()
    slots = tiles.shape[0]
    rows = N * ROWS

    def turn(c, slot):
        for s in range(N):
            block = g[c, s].reshape(rows, LANES)
            tiles[slot, :, pl.ds(s * rows, rows)] = block.T

    def sweep(base, out):
        def step(i, _):
            slot = lax.rem(i, slots)
            dst = out.at[pl.ds(pl.multiple_of(i * LANES, LANES), LANES)]
            copy = pltpu.make_async_copy(tiles.at[slot], dst, tile_sem.at[slot])

            @pl.when(i >= slots)
            def _():
                copy.wait()

            turn(base + i, slot)
            copy.start()
            return 0

        lax.fori_loop(0, FULL, step, 0)
        for i in range(FULL - slots, FULL):
            pltpu.make_async_copy(
                tiles.at[i % slots], out.at[pl.ds(i * LANES, LANES)], tile_sem.at[i % slots]
            ).wait()

    sweep(0, fg)
    sweep(FULL, fu)
    turn(BLOCKS - 1, 0)
    ends = [
        pltpu.make_async_copy(
            tiles.at[0, pl.ds(TAIL * i, TAIL)], out.at[pl.ds(FULL * LANES, TAIL)], tile_sem.at[i]
        )
        for i, out in enumerate((fg, fu))
    ]
    for copy in ends:
        copy.start()
    for copy in ends + others:
        copy.wait()


def local(train_gate, drift_gate, spread_gate, train_up, drift_up, spread_up, norm_train, norm_step):
    arrays = (train_gate, drift_gate, spread_gate, train_up, drift_up, spread_up)
    arrays += (norm_train.reshape(1, 20), norm_step.reshape(1, 20))
    depth = lax.axis_size(Z)
    wide = (ROWS, COLS)
    dma = pltpu.SemaphoreType.DMA
    g, rg, ru, cg, cu, norm = pl.pallas_call(
        gather_kernel,
        out_shape=(
            pltpu.VMEM((BLOCKS, N, N, ROWS, LANES), BF16),
            pltpu.VMEM(wide, F32),
            pltpu.VMEM(wide, F32),
            pltpu.VMEM((FULL + 1, LANES), F32),
            pltpu.VMEM((FULL + 1, LANES), F32),
            pltpu.VMEM((20, LANES), BF16),
        ),
        in_specs=[pl.BlockSpec(memory_space=pltpu.HBM)] * 8,
        out_specs=(pl.BlockSpec(memory_space=pltpu.VMEM),) * 6,
        scratch_shapes=[pltpu.VMEM(wide, F32)] * 6
        + [pltpu.VMEM((1, 20), F32)] * 2
        + [
            pltpu.VMEM((N * N, 24, LANES), F32),
            pltpu.VMEM((24, LANES), F32),
            pltpu.VMEM((depth, 8, LANES), F32),
            pltpu.VMEM((N * N, 8, LANES), F32),
            pltpu.VMEM((20, LANES), F32),
            dma((8,)),
            dma((2, N * N)),
            dma((2, N * N)),
            dma((depth,)),
            dma((depth,)),
            dma((N * N,)),
            dma((N * N,)),
            dma((4, 4)),
            dma((4, PAIRS, 4)),
        ],
        compiler_params=pltpu.CompilerParams(
            collective_id=0, has_side_effects=True, vmem_limit_bytes=24 * 2**20
        ),
        name="update_and_gather",
    )(*(pltpu.with_memory_space_constraint(a, pltpu.HBM) for a in arrays))
    turned = (COLS, N * N * ROWS)
    fg, fu, og, ou, cg, cu, serve = pl.pallas_call(
        write_kernel,
        out_shape=(jax.ShapeDtypeStruct(turned, BF16),) * 2
        + (jax.ShapeDtypeStruct(wide, F32),) * 2
        + (jax.ShapeDtypeStruct((FULL + 1, LANES), F32),) * 2
        + (jax.ShapeDtypeStruct((20, LANES), BF16),),
        in_specs=[pl.BlockSpec(memory_space=pltpu.VMEM)] * 6,
        out_specs=(pl.BlockSpec(memory_space=pltpu.HBM),) * 7,
        scratch_shapes=[pltpu.VMEM((4, LANES, N * N * ROWS), BF16), dma((5,)), dma((4,))],
        compiler_params=pltpu.CompilerParams(vmem_limit_bytes=16 * 2**20),
        name="turn_and_write",
    )(g, rg, ru, cg, cu, norm)
    return (
        fg.T, fu.T, cg.reshape(-1)[:COLS], cu.reshape(-1)[:COLS], serve.reshape(-1), og, ou,
    )


def solution(mesh):
    finer = Mesh(
        mesh.devices.reshape(mesh.shape["copy"], N, N, mesh.shape["cols"]), AXES
    )
    held = P(("copy", Y, X), Z)
    return jax.shard_map(
        local,
        mesh=finer,
        in_specs=(held,) * 6 + (P(AXES),) * 2,
        out_specs=(P("copy", Z), P("copy", Z), P(("copy", Z)), P(("copy", Z)), P("copy"), held, held),
        check_vma=False,
    )
```
